32 devices in a mesh: mp: 2 (over core), dev: 16 (over z, y, x).
Axes of the slice: x: 2, y: 2, z: 4, core: 2. Of those that a mesh axis runs over, the one named last changes fastest.
Arguments:
- spectrum: float32 [1024, 8192], P(None, ('mp', 'dev')), may hold values from 0.05 to 1
- water_mask: int32 [8192], P(('mp', 'dev')), may hold values 0 or 1
- courant: float32 [2, 1024], replicated, may hold values from 0.05 to 0.3
- stencil_sign: int32 [2, 1024], replicated, may hold values from 0 to 1
- quad_index: int32 [4, 1024, 2], replicated, may hold values from 0 to 1023
- quad_weight: float32 [4, 1024, 2], replicated, may hold values from 0.2 to 1
- nonlinear: float32 [1024], replicated, may hold values from 0.01 to 0.1
- stokes_table: bfloat16 [128, 1024], replicated, may hold values from -0.1875 to 0.1875
- point_index: int32 [4, 8192], P(None, ('mp', 'dev')), may hold values from 0 to 4095, as said below
- point_weight: float32 [4, 8192], P(None, ('mp', 'dev')), may hold values from 0.1 to 0.4
- ocean_index: int32 [4, 4096], P(None, ('mp', 'dev')), may hold values from 0 to 8191, as said below
- ocean_weight: float32 [4, 4096], P(None, ('mp', 'dev')), may hold values from 0.1 to 0.4
- currents: float32 [2, 64, 4096], P(None, None, ('mp', 'dev')), may hold values from -3 to 3
- coriolis: float32 [4096], P(('mp', 'dev')), may hold values from 0.2 to 0.6
- mixing: float32 [64], replicated, may hold values from 0.05 to 0.2
- surface_weights: float32 [64], replicated, may hold values from 0.005 to 0.05
Outputs:
- spectrum_out: float32 [1024, 8192], P(None, ('mp', 'dev'))
- currents_out: float32 [2, 64, 4096], P(None, None, ('mp', 'dev'))
The draws below stay inside these ranges and needn't reach their ends.
Inputs may be any that keep to these rules, and one draw needn't show every extreme that they name: `point_index`: entry j of point p names an ocean cell in row p // 256 plus -1, 0 or 1 and column (p % 256) // 2 plus -1, 0 or 1, both wrapping. `ocean_index`: entry j of cell c names a wave point in row c // 128 plus -1, 0 or 1 and column 2 (c % 128) plus -2 to 3, both wrapping.
All inputs are finite; a program needn't handle non-finite values. No bound on the sum of `water_mask` on one device may be relied on, other than what follows from the above.
Results may differ from the reference program's by a relative error of at most 0.0003.
The reference program's roundings to bfloat16 on the way count: a program that leaves them out, or rounds other values in their place, can miss the bound.
Values sent between devices are 32-bit elements; how exact they have to be, the bound alone decides.
A program may use at most 64 MiB of HBM per device.

```python
import math
import jax
import jax.numpy as jnp
from jax import lax

K = 1024
L = 64
MX = 256
STEPS = 2
OX = 128
MY = 32
P_SIZE = 8192
NOC = 4096


def draw_point_index(key, part):
    point_total = MX * MY
    position = jnp.arange(point_total, dtype=jnp.int32)
    row_key, column_key = jax.random.split(jax.random.fold_in(key, 11))
    row_pick = (position // MX)[None, :] + jax.random.randint(row_key, (4, point_total), -1, 2)
    column_pick = (position % MX // 2)[None, :] + jax.random.randint(column_key, (4, point_total), -1, 2)
    return (jnp.mod(row_pick, MY) * OX + jnp.mod(column_pick, OX)).astype(jnp.int32)


def draw_ocean_index(key, part):
    cell_total = OX * MY
    position = jnp.arange(cell_total, dtype=jnp.int32)
    row_key, column_key = jax.random.split(jax.random.fold_in(key, 23))
    row_pick = (position // OX)[None, :] + jax.random.randint(row_key, (4, cell_total), -1, 2)
    column_pick = (2 * (position % OX))[None, :] + jax.random.randint(column_key, (4, cell_total), -2, 4)
    return (jnp.mod(row_pick, MY) * MX + jnp.mod(column_pick, MX)).astype(jnp.int32)


def place_ends(drawn, stream_key, low, high):
    place = [jax.random.randint(jax.random.fold_in(stream_key, axis), (), 0, length) for axis, length in enumerate(drawn.shape)]
    longest = drawn.shape.index(max(drawn.shape))
    beside = place[:longest] + [(place[longest] + 1) % drawn.shape[longest]] + place[longest + 1:]
    return drawn.at[tuple(place)].set(low).at[tuple(beside)].set(high)


def block_levels(rng, extent, cuts, smallest, top_value):
    def one(dim, parts):
        steps = jax.random.uniform(jax.random.fold_in(jax.random.fold_in(rng, 6), dim), (parts,), jnp.float32, smallest / len(cuts), top_value / len(cuts))
        return jnp.repeat(jnp.exp(steps), extent[dim] // parts).reshape((-1,) + (1,) * (len(extent) - dim - 1))

    level = one(*cuts[0])
    for cut in cuts[1:]:
        level = level * one(*cut)
    return level


def noise(own_key, extent, deviation, bound, cuts=(), held_as=jnp.bfloat16):
    factor_of = block_levels(own_key, extent, cuts, -0.22, 0.18) if cuts else 1.0
    values = jax.random.normal(own_key, extent, jnp.float32) * deviation * factor_of
    return jnp.minimum(jnp.maximum(values, -bound), bound).astype(held_as)


def setup_inputs(seed: int = 0) -> dict:
    key_of = jax.random.split(jax.random.key(seed), 17)
    spectrum = jnp.clip(jnp.exp(math.log(1.0) - 2.9957323 * jax.random.uniform(key_of[0], (K, P_SIZE), jnp.float32) ** block_levels(key_of[0], (K, P_SIZE), ((1, 32),), -0.2, 0.2)), 0.05, 1.0)
    water_mask = place_ends((jax.random.randint(key_of[1], (P_SIZE,), 0, 8) < 7).astype(jnp.int32), jax.random.fold_in(key_of[1], 1), 0, 1)
    courant = jnp.clip(jnp.exp(jax.random.uniform(key_of[2], (2, K), jnp.float32, math.log(0.05), math.log(0.3))), 0.05, 0.3)
    stencil_sign = place_ends(jax.random.randint(key_of[3], (2, K), 0, 2), jax.random.fold_in(key_of[3], 1), 0, 1).astype(jnp.int32)
    quad_index = place_ends(jax.random.randint(key_of[4], (4, K, 2), 0, K), jax.random.fold_in(key_of[4], 1), 0, K - 1).astype(jnp.int32)
    quad_weight = jnp.clip(jax.random.uniform(key_of[5], (4, K, 2), jnp.float32, 0.2, 1.0), 0.2, 1.0)
    nonlinear = jnp.clip(jnp.exp(jax.random.uniform(key_of[6], (K,), jnp.float32, math.log(0.01), math.log(0.1))), 0.01, 0.1)
    stokes_table = noise(key_of[7], (2 * L, K), K ** -0.5, 0.1875)
    point_index = draw_point_index(jax.random.fold_in(key_of[16], 71), 0)
    point_weight = jnp.clip(0.1 + 0.3 * jax.random.uniform(key_of[9], (4, P_SIZE), jnp.float32) ** block_levels(key_of[9], (4, P_SIZE), ((1, 32),), -0.2, 0.2), 0.1, 0.4)
    ocean_index = draw_ocean_index(jax.random.fold_in(key_of[16], 71), 0)
    ocean_weight = jnp.clip(0.1 + 0.3 * jax.random.uniform(key_of[11], (4, NOC), jnp.float32) ** block_levels(key_of[11], (4, NOC), ((1, 32),), -0.2, 0.2), 0.1, 0.4)
    currents = noise(key_of[12], (2, L, NOC), 0.5, 3.0, ((2, 32),), jnp.float32)
    coriolis = jnp.clip(0.2 + 0.400000021 * jax.random.uniform(key_of[13], (NOC,), jnp.float32) ** block_levels(key_of[13], (NOC,), ((0, 32),), -0.2, 0.2), 0.2, 0.6)
    mixing = jnp.clip(jax.random.uniform(key_of[14], (L,), jnp.float32, 0.05, 0.2), 0.05, 0.2)
    surface_weights = jnp.clip(jnp.exp(jax.random.uniform(key_of[15], (L,), jnp.float32, math.log(0.005), math.log(0.05))), 0.005, 0.05)
    return dict(spectrum=spectrum, water_mask=water_mask, courant=courant, stencil_sign=stencil_sign, quad_index=quad_index, quad_weight=quad_weight, nonlinear=nonlinear, stokes_table=stokes_table, point_index=point_index, point_weight=point_weight, ocean_index=ocean_index, ocean_weight=ocean_weight, currents=currents, coriolis=coriolis, mixing=mixing, surface_weights=surface_weights)


ocean_step_size = 0.5


def advect(spectra, padded, point_flow, courant, stencil_sign):
    eastward = stencil_sign[0][:, None, None] == 1
    northward = stencil_sign[1][:, None, None] == 1
    sense_x = (2 * stencil_sign[0] - 1).astype(jnp.float32)[:, None, None]
    sense_y = (2 * stencil_sign[1] - 1).astype(jnp.float32)[:, None, None]
    behind_x = jnp.where(eastward, jnp.roll(spectra, 1, axis=2), jnp.roll(spectra, -1, axis=2))
    behind_y = jnp.where(northward, padded[:, :-2], padded[:, 2:])
    speed_x = courant[0][:, None, None] * (1.0 + 0.5 * jnp.tanh(sense_x * point_flow[0][None]))
    speed_y = courant[1][:, None, None] * (1.0 + 0.5 * jnp.tanh(sense_y * point_flow[1][None]))
    return spectra - speed_x * (spectra - behind_x) - speed_y * (spectra - behind_y)


def nonlinear_update(advected, interps, gain_rows, wet_row):
    total_sum = interps[0] + interps[1] + interps[2] + interps[3]
    pair_sum = interps[0] * interps[1] + interps[2] * interps[3]
    source = advected * advected * total_sum - advected * pair_sum
    return wet_row[None, :] * (advected + gain_rows[:, None] * source)


def vertical_mix(profile, mixing):
    above_level = jnp.concatenate([profile[:1], profile[:-1]], axis=0)
    below_level = jnp.concatenate([profile[1:], profile[-1:]], axis=0)
    return mixing[:, None, None] * (above_level - 2.0 * profile + below_level)


def ocean_tendency(zonal_flow, meridional, padded_zonal, mixing):
    vorticity = 0.5 * (jnp.roll(meridional, -1, axis=2) - jnp.roll(meridional, 1, axis=2)) - 0.5 * (padded_zonal[:, 2:] - padded_zonal[:, :-2])
    return vorticity, vertical_mix(zonal_flow, mixing), vertical_mix(meridional, mixing)


def ocean_advance(zonal_flow, meridional, tendency, stokes_drift, rotation):
    vorticity, mix_zonal, mix_meridional = tendency
    drift_x = stokes_drift[0]
    drift_y = stokes_drift[1]
    new_zonal = zonal_flow + ocean_step_size * (rotation[None] * (meridional + drift_y) + vorticity * drift_y + mix_zonal)
    new_meridional = meridional + ocean_step_size * (-rotation[None] * (zonal_flow + drift_x) - vorticity * drift_x + mix_meridional)
    return jnp.stack([new_zonal, new_meridional])


def reference(spectrum, water_mask, courant, stencil_sign, quad_index, quad_weight, nonlinear, stokes_table, point_index, point_weight, ocean_index, ocean_weight, currents, coriolis, mixing, surface_weights):
    repeated = quad_index[:, :, 0] == quad_index[:, :, 1]
    first_weight = jnp.where(repeated, quad_weight[:, :, 0] + quad_weight[:, :, 1], quad_weight[:, :, 0]).astype(jnp.bfloat16).astype(jnp.float32)
    second_weight = jnp.where(repeated, jnp.zeros_like(quad_weight[:, :, 1]), quad_weight[:, :, 1]).astype(jnp.bfloat16).astype(jnp.float32)
    first_index = quad_index[:, :, 0]
    second_index = quad_index[:, :, 1]
    wet_points = water_mask.astype(jnp.float32)
    stokes_rows = stokes_table.astype(jnp.float32)
    rotation = coriolis.reshape(MY, OX)
    ocean_state = currents
    spectra = spectrum
    for step_index in range(STEPS):
        surface = jnp.sum(surface_weights[None, :, None] * ocean_state, axis=1)
        point_flow = sum(point_weight[config][None, :] * surface[:, point_index[config]] for config in range(4))
        map_grid = spectra.reshape(K, MY, MX)
        padded = jnp.concatenate([map_grid[:, -1:], map_grid, map_grid[:, :1]], axis=1)
        advected = advect(map_grid, padded, point_flow.reshape(2, MY, MX), courant, stencil_sign)
        rounded = lax.optimization_barrier(advected.astype(jnp.bfloat16)).astype(jnp.float32)

        def one_block(pieces):
            block_rows, block_rounded, block_wet = pieces
            interps = first_weight[:, :, None] * block_rounded[first_index] + second_weight[:, :, None] * block_rounded[second_index]
            return nonlinear_update(block_rows, interps, nonlinear, block_wet)

        updated = lax.map(one_block, (advected.transpose(1, 0, 2), rounded.transpose(1, 0, 2), wet_points.reshape(MY, MX)))
        spectra = updated.transpose(1, 0, 2).reshape(K, MY * MX)
        spectra_rounded = lax.optimization_barrier(spectra.astype(jnp.bfloat16)).astype(jnp.float32)
        stokes = jnp.dot(stokes_rows, spectra_rounded, precision=lax.Precision.HIGHEST)
        stokes_drift = sum(ocean_weight[config][None, :] * stokes[:, ocean_index[config]] for config in range(4))
        stokes_drift = stokes_drift.reshape(2, L, MY, OX)
        zonal_flow = ocean_state[0].reshape(L, MY, OX)
        meridional = ocean_state[1].reshape(L, MY, OX)
        padded_zonal = jnp.concatenate([zonal_flow[:, -1:], zonal_flow, zonal_flow[:, :1]], axis=1)
        tendency = ocean_tendency(zonal_flow, meridional, padded_zonal, mixing)
        ocean_state = ocean_advance(zonal_flow, meridional, tendency, stokes_drift, rotation).reshape(2, L, MY * OX)
    return spectra, ocean_state
```

```python
import jax
import jax.numpy as jnp
from jax import lax
from jax.experimental import pallas as pl
from jax.experimental.pallas import tpu as pltpu
from jax.sharding import PartitionSpec as P

STEPS = 2
OCEAN_STEP = 0.5
COMM = 8
BLOCKS = 4
MESH = pl.DeviceIdType.MESH
HIGH = lax.Precision.HIGHEST


def wave_kernel(
    spec, wet, courant, sign, qidx, qwt, nonlinear, table, pidx, pwt, oidx, owt,
    currents, coriolis, mixing, sweight,
    spec_out, cur_out,
    araw, cols, quad, near, far, adv, advb, mid, midb, state,
    sflow, shalo, zhalo, obuf, ohalo, ptab, otab, dbuf, dhalo, dself, tan,
    sem1s, sem1r, sem2s, sem2r, ssend, srecv, zsend, zrecv, osend, orecv, dsend, drecv,
):
    comps, points = spec.shape
    cells = coriolis.shape[1]
    levels = mixing.shape[1]
    dev_count = lax.axis_size("dev")
    total = lax.axis_size("mp") * dev_count
    pos = lax.axis_index("mp") * dev_count + lax.axis_index("dev")
    odd = lax.rem(pos, 2)
    up = lax.rem(pos + 1, total)
    down = lax.rem(pos + total - 1, total)
    up2 = lax.rem(pos + 2, total)
    down2 = lax.rem(pos + total - 2, total)
    partner = pos + 1 - 2 * odd
    far_to = lax.rem(pos + 2 - 4 * odd + total, total)

    def where_is(p):
        return (lax.div(p, dev_count), lax.rem(p, dev_count))

    def remote(src, dst, ssem, rsem, p):
        return pltpu.make_async_remote_copy(
            src_ref=src, dst_ref=dst, send_sem=ssem, recv_sem=rsem,
            device_id=where_is(p), device_id_type=MESH,
        )

    size = comps // COMM

    def rows(c):
        return pl.ds(pl.multiple_of(c * size, size), size)

    def swap(step, c):
        src = spec if step == 0 else mid
        return remote(src.at[rows(c)], near.at[step, rows(c)], sem1s.at[step, c], sem1r.at[step, c], partner)

    def relay(step, c):
        return remote(near.at[step, rows(c)], far.at[step, rows(c)], sem2s.at[step, c], sem2r.at[step, c], far_to)

    def pair(src_up, src_down, halo, ssem, rsem, step):
        return (
            remote(src_up, halo.at[step, 0], ssem.at[step, 0], rsem.at[step, 0], up),
            remote(src_down, halo.at[step, 1], ssem.at[step, 1], rsem.at[step, 1], down),
        )

    def surface_pair(step):
        return pair(sflow.at[step], sflow.at[step], shalo, ssend, srecv, step)

    def zonal_pair(step):
        src = currents.at[0] if step == 0 else state.at[0]
        return pair(src, src, zhalo, zsend, zrecv, step)

    def index_pair():
        return pair(obuf, obuf, ohalo, osend, orecv, 0)

    def drift_pair(step):
        return pair(dbuf.at[step, 0], dbuf.at[step, 1], dhalo, dsend, drecv, step)

    def start(copies):
        for copy in copies:
            copy.start()

    def received(copies):
        for copy in copies:
            copy.wait_recv()

    def sent(copies):
        for copy in copies:
            copy.wait_send()

    def each(low, high, body):
        def run(c, carry):
            body(c)
            return carry

        lax.fori_loop(low, high, run, 0)

    barrier = pltpu.get_barrier_semaphore()
    for p in (up, down, up2, down2):
        pl.semaphore_signal(barrier, inc=1, device_id=where_is(p), device_id_type=MESH)
    pl.semaphore_wait(barrier, 4)

    each(0, COMM, lambda c: swap(0, c).start())
    start(zonal_pair(0))
    obuf[0:4, :] = oidx[...].astype(jnp.float32)
    obuf[4:8, :] = owt[...]

    araw[...] = jnp.zeros_like(araw)
    araw[0:2, :] = courant[...]
    araw[2:4, :] = (2 * sign[...] - 1).astype(jnp.float32)
    araw[4:5, :] = nonlinear[...]
    araw[5:6, 0:levels] = mixing[...]
    araw[6:7, 0:levels] = sweight[...]
    araw[8:16, :] = qidx[...].astype(jnp.float32)
    araw[16:24, :] = qwt[...]
    cols[...] = jnp.transpose(araw[...])
    sflow[...] = jnp.zeros_like(sflow)
    level_mix = cols[0:levels, 5:6]
    level_weight = cols[0:levels, 6:7]

    def surface(source, step):
        for a in range(2):
            sflow[step, a : a + 1, :] = jnp.sum(level_weight * source[a], axis=0, keepdims=True)

    surface(currents, 0)
    start(index_pair())
    start(surface_pair(0))

    lanes = lax.broadcasted_iota(jnp.int32, (32, comps), 1).astype(jnp.float32)

    def build_quad(c):
        for sub in range(size // 32):
            at = pl.ds(pl.multiple_of(c * size + sub * 32, 32), 32)
            col = cols[at, :]
            for j in range(4):
                one = jnp.where(col[:, 8 + 2 * j : 9 + 2 * j] == lanes, col[:, 16 + 2 * j : 17 + 2 * j], 0.0)
                two = jnp.where(col[:, 9 + 2 * j : 10 + 2 * j] == lanes, col[:, 17 + 2 * j : 18 + 2 * j], 0.0)
                quad[j, at, :] = (one + two).astype(jnp.bfloat16)

    def forward(step):
        def body(c):
            swap(step, c).wait_recv()
            relay(step, c).start()

        return body

    def first(c):
        build_quad(c)
        forward(0)(c)

    each(0, COMM, first)

    slots = lax.broadcasted_iota(jnp.int32, (cells, points), 0)
    for q, owner in enumerate((down, pos, up)):
        acc = jnp.zeros((cells, points), jnp.float32)
        for j in range(4):
            acc = acc + jnp.where(pidx[j : j + 1, :] - owner * cells == slots, pwt[j : j + 1, :], 0.0)
        ptab[q] = acc
    received(index_pair())
    oslots = lax.broadcasted_iota(jnp.int32, (points, cells), 0).astype(jnp.float32)
    base = (pos * points).astype(jnp.float32)
    for q in range(3):
        source = obuf[...] if q == 2 else ohalo[0, q]
        acc = jnp.zeros((points, cells), jnp.float32)
        for j in range(4):
            acc = acc + jnp.where(source[j : j + 1, :] - base == oslots, source[4 + j : 5 + j, :], 0.0)
        otab[q] = acc

    parity = (1 - 2 * odd).astype(jnp.float32)

    def flow(step):
        received(surface_pair(step))
        total_flow = jnp.dot(shalo[step, 0], ptab[0], precision=HIGH, preferred_element_type=jnp.float32)
        total_flow += jnp.dot(sflow[step], ptab[1], precision=HIGH, preferred_element_type=jnp.float32)
        total_flow += jnp.dot(shalo[step, 1], ptab[2], precision=HIGH, preferred_element_type=jnp.float32)
        tan[...] = jnp.tanh(total_flow)

    def advect(step):
        source = spec if step == 0 else mid

        def body(c):
            relay(step, c).wait_recv()
            at = rows(c)
            own = source[at, :]
            col = cols[at, :]
            sense_x = col[:, 2:3]
            sense_y = col[:, 3:4]
            behind_x = jnp.where(sense_x > 0, pltpu.roll(own, 1, 1), pltpu.roll(own, points - 1, 1))
            behind_y = jnp.where(sense_y * parity > 0, far[step, at, :], near[step, at, :])
            speed_x = col[:, 0:1] * (1.0 + 0.5 * (sense_x * tan[0:1, :]))
            speed_y = col[:, 1:2] * (1.0 + 0.5 * (sense_y * tan[1:2, :]))
            value = own - speed_x * (own - behind_x) - speed_y * (own - behind_y)
            adv[at, :] = value
            advb[at, :] = value.astype(jnp.bfloat16)

        each(0, COMM, body)

    wide = comps // BLOCKS
    wet_row = wet[...].astype(jnp.float32)

    def source_block(step):
        target = mid if step == 0 else spec_out

        def body(r):
            at = pl.ds(pl.multiple_of(r * wide, wide), wide)
            terms = [
                jnp.dot(quad[j, at, :], advb[...], preferred_element_type=jnp.float32) for j in range(4)
            ]
            value = adv[at, :]
            total_sum = terms[0] + terms[1] + terms[2] + terms[3]
            pair_sum = terms[0] * terms[1] + terms[2] * terms[3]
            new = wet_row * (value + cols[at, 4:5] * (value * value * total_sum - value * pair_sum))
            target[at, :] = new
            midb[at, :] = new.astype(jnp.bfloat16)

        return body

    def drift_parts(step):
        stokes = jnp.dot(table[...], midb[...], preferred_element_type=jnp.float32)
        dbuf[step, 0] = jnp.dot(stokes, otab[1], precision=HIGH, preferred_element_type=jnp.float32)
        dbuf[step, 1] = jnp.dot(stokes, otab[0], precision=HIGH, preferred_element_type=jnp.float32)
        start(drift_pair(step))
        dself[...] = jnp.dot(stokes, otab[2], precision=HIGH, preferred_element_type=jnp.float32)

    level_row = lax.broadcasted_iota(jnp.int32, (levels, cells), 0)

    def mix(w):
        above = jnp.where(level_row == 0, w, pltpu.roll(w, 1, 0))
        below = jnp.where(level_row == levels - 1, w, pltpu.roll(w, levels - 1, 0))
        return level_mix * (above - 2.0 * w + below)

    def ocean(step):
        received(drift_pair(step))
        received(zonal_pair(step))
        source = currents if step == 0 else state
        target = state if step == 0 else cur_out
        drift = dself[...] + dhalo[step, 0] + dhalo[step, 1]
        drift_x, drift_y = drift[0:levels], drift[levels : 2 * levels]
        u, v = source[0], source[1]
        rot = coriolis[...]
        turn = 0.5 * (pltpu.roll(v, cells - 1, 1) - pltpu.roll(v, 1, 1)) - 0.5 * (zhalo[step, 1] - zhalo[step, 0])
        new_u = u + OCEAN_STEP * (rot * (v + drift_y) + turn * drift_y + mix(u))
        new_v = v + OCEAN_STEP * (-rot * (u + drift_x) - turn * drift_x + mix(v))
        target[0] = new_u
        target[1] = new_v

    flow(0)
    advect(0)
    source_block(0)(0)
    per = COMM // BLOCKS
    each(0, per, lambda c: swap(1, c).start())
    each(1, BLOCKS, source_block(0))
    drift_parts(0)
    each(per, COMM, lambda c: swap(1, c).start())
    each(0, COMM - 3, forward(1))
    ocean(0)
    surface(state, 1)
    start(surface_pair(1))
    start(zonal_pair(1))
    each(COMM - 3, COMM, forward(1))
    flow(1)
    advect(1)
    each(0, BLOCKS, source_block(1))
    drift_parts(1)
    ocean(1)

    sent(index_pair())
    for step in range(STEPS):
        each(0, COMM, lambda c: swap(step, c).wait_send())
        each(0, COMM, lambda c: relay(step, c).wait_send())
        sent(surface_pair(step))
        sent(zonal_pair(step))
        sent(drift_pair(step))


def local(
    spectrum, water_mask, courant, stencil_sign, quad_index, quad_weight, nonlinear, stokes_table,
    point_index, point_weight, ocean_index, ocean_weight, currents, coriolis, mixing, surface_weights,
):
    comps, points = spectrum.shape
    levels, cells = currents.shape[1:]
    f32, bf16 = jnp.float32, jnp.bfloat16
    vm = pl.BlockSpec(memory_space=pltpu.VMEM)
    dma = pltpu.SemaphoreType.DMA
    scratch = [
        pltpu.VMEM((128, comps), f32),
        pltpu.VMEM((comps, 128), f32),
        pltpu.VMEM((4, comps, comps), bf16),
        pltpu.VMEM((STEPS, comps, points), f32),
        pltpu.VMEM((STEPS, comps, points), f32),
        pltpu.VMEM((comps, points), f32),
        pltpu.VMEM((comps, points), bf16),
        pltpu.VMEM((comps, points), f32),
        pltpu.VMEM((comps, points), bf16),
        pltpu.VMEM((2, levels, cells), f32),
        pltpu.VMEM((STEPS, 8, cells), f32),
        pltpu.VMEM((STEPS, 2, 8, cells), f32),
        pltpu.VMEM((STEPS, 2, levels, cells), f32),
        pltpu.VMEM((8, cells), f32),
        pltpu.VMEM((1, 2, 8, cells), f32),
        pltpu.VMEM((3, cells, points), f32),
        pltpu.VMEM((3, points, cells), f32),
        pltpu.VMEM((STEPS, 2, 2 * levels, cells), f32),
        pltpu.VMEM((STEPS, 2, 2 * levels, cells), f32),
        pltpu.VMEM((2 * levels, cells), f32),
        pltpu.VMEM((8, points), f32),
        dma((STEPS, COMM)),
        dma((STEPS, COMM)),
        dma((STEPS, COMM)),
        dma((STEPS, COMM)),
    ] + [dma((n, 2)) for n in (STEPS, STEPS, STEPS, STEPS, 1, 1, STEPS, STEPS)]
    return pl.pallas_call(
        wave_kernel,
        out_shape=(
            jax.ShapeDtypeStruct((comps, points), f32),
            jax.ShapeDtypeStruct(currents.shape, f32),
        ),
        in_specs=[vm] * 16,
        out_specs=(vm, vm),
        scratch_shapes=scratch,
        compiler_params=pltpu.CompilerParams(
            collective_id=0, has_side_effects=True, vmem_limit_bytes=56 * 1024 * 1024
        ),
    )(
        spectrum,
        water_mask.reshape(1, points),
        courant,
        stencil_sign,
        quad_index.transpose(0, 2, 1).reshape(8, comps),
        quad_weight.transpose(0, 2, 1).reshape(8, comps),
        nonlinear.reshape(1, comps),
        stokes_table,
        point_index,
        point_weight,
        ocean_index,
        ocean_weight,
        currents,
        coriolis.reshape(1, cells),
        mixing.reshape(1, levels),
        surface_weights.reshape(1, levels),
    )


def solution(mesh):
    ring = P(("mp", "dev"))
    split = P(None, ("mp", "dev"))
    deep = P(None, None, ("mp", "dev"))
    return jax.shard_map(
        local,
        mesh=mesh,
        in_specs=(
            split, ring, P(), P(), P(), P(), P(), P(), split, split, split, split, deep, ring, P(), P(),
        ),
        out_specs=(split, deep),
        check_vma=False,
    )
```

```python
import jax
import jax.numpy as jnp
from jax import lax
from jax.experimental import pallas as pl
from jax.experimental.pallas import tpu as pltpu
from jax.sharding import PartitionSpec as P

STEPS = 2
OCEAN_STEP = 0.5
COMM = 16
BLOCKS = 4
MESH = pl.DeviceIdType.MESH
HIGH = lax.Precision.HIGHEST


def wave_kernel(
    spec, wet, courant, sign, qidx, qwt, nonlinear, table, pidx, pwt, oidx, owt,
    currents, coriolis, mixing, sweight,
    spec_out, cur_out,
    araw, cols, quad, near, far, adv, advb, mid, midb, state,
    sflow, shalo, zhalo, obuf, ohalo, ptab, otab, dbuf, dhalo, dself, tan, acc,
    sem1s, sem1r, sem2s, sem2r, ssend, srecv, zsend, zrecv, osend, orecv, dsend, drecv,
):
    comps, points = spec.shape
    cells = coriolis.shape[1]
    levels = mixing.shape[1]
    dev_count = lax.axis_size("dev")
    total = lax.axis_size("mp") * dev_count
    pos = lax.axis_index("mp") * dev_count + lax.axis_index("dev")
    odd = lax.rem(pos, 2)
    up = lax.rem(pos + 1, total)
    down = lax.rem(pos + total - 1, total)
    up2 = lax.rem(pos + 2, total)
    down2 = lax.rem(pos + total - 2, total)
    partner = pos + 1 - 2 * odd
    far_to = lax.rem(pos + 2 - 4 * odd + total, total)

    def where_is(p):
        return (lax.div(p, dev_count), lax.rem(p, dev_count))

    def remote(src, dst, ssem, rsem, p):
        return pltpu.make_async_remote_copy(
            src_ref=src, dst_ref=dst, send_sem=ssem, recv_sem=rsem,
            device_id=where_is(p), device_id_type=MESH,
        )

    size = comps // COMM

    def rows(c):
        return pl.ds(pl.multiple_of(c * size, size), size)

    def swap(step, c):
        src = spec if step == 0 else mid
        return remote(src.at[rows(c)], near.at[step, rows(c)], sem1s.at[step, c], sem1r.at[step, c], partner)

    def relay(step, c):
        return remote(near.at[step, rows(c)], far.at[step, rows(c)], sem2s.at[step, c], sem2r.at[step, c], far_to)

    def pair(src_up, src_down, halo, ssem, rsem, step):
        return (
            remote(src_up, halo.at[step, 0], ssem.at[step, 0], rsem.at[step, 0], up),
            remote(src_down, halo.at[step, 1], ssem.at[step, 1], rsem.at[step, 1], down),
        )

    def surface_pair(step):
        return pair(sflow.at[step], sflow.at[step], shalo, ssend, srecv, step)

    def zonal_pair(step):
        src = currents.at[0] if step == 0 else state.at[0]
        return pair(src, src, zhalo, zsend, zrecv, step)

    def index_pair():
        return pair(obuf, obuf, ohalo, osend, orecv, 0)

    def drift_pair(step):
        return pair(dbuf.at[step, 0], dbuf.at[step, 1], dhalo, dsend, drecv, step)

    def start(copies):
        for copy in copies:
            copy.start()

    def received(copies):
        for copy in copies:
            copy.wait_recv()

    def sent(copies):
        for copy in copies:
            copy.wait_send()

    def each(low, high, body):
        def run(c, carry):
            body(c)
            return carry

        lax.fori_loop(low, high, run, 0)

    barrier = pltpu.get_barrier_semaphore()
    for p in (up, down, up2, down2):
        pl.semaphore_signal(barrier, inc=1, device_id=where_is(p), device_id_type=MESH)
    pl.semaphore_wait(barrier, 4)

    each(0, COMM, lambda c: swap(0, c).start())
    start(zonal_pair(0))
    obuf[0:4, :] = oidx[...].astype(jnp.float32)
    obuf[4:8, :] = owt[...]

    araw[...] = jnp.zeros_like(araw)
    araw[0:2, :] = courant[...]
    araw[2:4, :] = (2 * sign[...] - 1).astype(jnp.float32)
    araw[4:5, :] = nonlinear[...]
    araw[5:6, 0:levels] = mixing[...]
    araw[6:7, 0:levels] = sweight[...]
    for j in range(4):
        araw[8 + 2 * j : 10 + 2 * j, :] = qidx[j].astype(jnp.float32)
        araw[16 + 2 * j : 18 + 2 * j, :] = qwt[j]
    cols[...] = jnp.transpose(araw[...])
    sflow[...] = jnp.zeros_like(sflow)
    level_mix = cols[0:levels, 5:6]
    level_weight = cols[0:levels, 6:7]

    def surface(source, step):
        for a in range(2):
            sflow[step, a : a + 1, :] = jnp.sum(level_weight * source[a], axis=0, keepdims=True)

    surface(currents, 0)
    start(index_pair())
    start(surface_pair(0))

    lanes = lax.broadcasted_iota(jnp.int32, (32, comps), 1).astype(jnp.float32)

    def build_quad(c):
        for sub in range(2 * size // 32):
            at = pl.ds(pl.multiple_of(c * 2 * size + sub * 32, 32), 32)
            col = cols[at, :]
            for j in range(4):
                one = jnp.where(col[:, 8 + 2 * j : 9 + 2 * j] == lanes, col[:, 16 + 2 * j : 17 + 2 * j], 0.0)
                two = jnp.where(col[:, 9 + 2 * j : 10 + 2 * j] == lanes, col[:, 17 + 2 * j : 18 + 2 * j], 0.0)
                quad[j, at, :] = (one + two).astype(jnp.bfloat16)

    def forward(step):
        def body(c):
            swap(step, c).wait_recv()
            relay(step, c).start()

        return body

    def first(c):
        build_quad(c)
        forward(0)(c)

    each(0, COMM // 2, first)

    slots = lax.broadcasted_iota(jnp.int32, (cells, points), 0)
    for q, owner in enumerate((down, pos, up)):
        spread = jnp.zeros((cells, points), jnp.float32)
        for j in range(4):
            spread = spread + jnp.where(pidx[j : j + 1, :] - owner * cells == slots, pwt[j : j + 1, :], 0.0)
        ptab[q] = spread
    received(index_pair())
    oslots = lax.broadcasted_iota(jnp.int32, (points, cells), 0).astype(jnp.float32)
    base = (pos * points).astype(jnp.float32)
    for q in range(3):
        source = obuf[...] if q == 2 else ohalo[0, q]
        spread = jnp.zeros((points, cells), jnp.float32)
        for j in range(4):
            spread = spread + jnp.where(source[j : j + 1, :] - base == oslots, source[4 + j : 5 + j, :], 0.0)
        otab[q] = spread

    parity = (1 - 2 * odd).astype(jnp.float32)

    def flow(step):
        received(surface_pair(step))
        total_flow = jnp.dot(shalo[step, 0], ptab[0], precision=HIGH, preferred_element_type=jnp.float32)
        total_flow += jnp.dot(sflow[step], ptab[1], precision=HIGH, preferred_element_type=jnp.float32)
        total_flow += jnp.dot(shalo[step, 1], ptab[2], precision=HIGH, preferred_element_type=jnp.float32)
        tan[...] = jnp.tanh(total_flow)

    wide = comps // BLOCKS
    per = COMM // BLOCKS
    wet_row = wet[...].astype(jnp.float32)

    def block(r):
        return pl.ds(pl.multiple_of(r * wide, wide), wide)

    def advect(step):
        source = spec if step == 0 else mid

        def body(c):
            relay(step, c).wait_recv()
            at = rows(c)
            own = source[at, :]
            col = cols[at, :]
            sense_x = col[:, 2:3]
            sense_y = col[:, 3:4]
            behind_x = jnp.where(sense_x > 0, pltpu.roll(own, 1, 1), pltpu.roll(own, points - 1, 1))
            behind_y = jnp.where(sense_y * parity > 0, far[step, at, :], near[step, at, :])
            speed_x = col[:, 0:1] * (1.0 + 0.5 * (sense_x * tan[0:1, :]))
            speed_y = col[:, 1:2] * (1.0 + 0.5 * (sense_y * tan[1:2, :]))
            value = own - speed_x * (own - behind_x) - speed_y * (own - behind_y)
            adv[at, :] = value
            advb[at, :] = value.astype(jnp.bfloat16)

        return body

    def gather(step, g):
        each(g * per, (g + 1) * per, advect(step))
        part = advb[g * wide : (g + 1) * wide, :]

        def body(r):
            at = block(r)
            for j in range(4):
                term = jnp.dot(
                    quad[j, at, g * wide : (g + 1) * wide], part, preferred_element_type=jnp.float32
                )
                if g == 0:
                    acc[j, at, :] = term
                else:
                    acc[j, at, :] += term

        each(0, BLOCKS, body)

    def finish(step):
        target = mid if step == 0 else spec_out

        def body(r):
            at = rows(r)
            terms = [acc[j, at, :] for j in range(4)]
            value = adv[at, :]
            total_sum = terms[0] + terms[1] + terms[2] + terms[3]
            pair_sum = terms[0] * terms[1] + terms[2] * terms[3]
            new = wet_row * (value + cols[at, 4:5] * (value * value * total_sum - value * pair_sum))
            target[at, :] = new
            midb[at, :] = new.astype(jnp.bfloat16)

        return body

    def drift_parts(step):
        stokes = jnp.dot(table[...], midb[...], preferred_element_type=jnp.float32)
        ahead, behind = drift_pair(step)
        dbuf[step, 0] = jnp.dot(stokes, otab[1], precision=HIGH, preferred_element_type=jnp.float32)
        ahead.start()
        dbuf[step, 1] = jnp.dot(stokes, otab[0], precision=HIGH, preferred_element_type=jnp.float32)
        behind.start()
        dself[...] = jnp.dot(stokes, otab[2], precision=HIGH, preferred_element_type=jnp.float32)

    level_row = lax.broadcasted_iota(jnp.int32, (levels, cells), 0)

    def mix(w):
        above = jnp.where(level_row == 0, w, pltpu.roll(w, 1, 0))
        below = jnp.where(level_row == levels - 1, w, pltpu.roll(w, levels - 1, 0))
        return level_mix * (above - 2.0 * w + below)

    def ocean(step):
        source = currents if step == 0 else state
        target = state if step == 0 else cur_out
        received(zonal_pair(step))
        u, v = source[0], source[1]
        rot = coriolis[...]
        turn = 0.5 * (pltpu.roll(v, cells - 1, 1) - pltpu.roll(v, 1, 1)) - 0.5 * (zhalo[step, 1] - zhalo[step, 0])
        mix_u, mix_v = mix(u), mix(v)
        received(drift_pair(step))
        drift = dself[...] + dhalo[step, 0] + dhalo[step, 1]
        drift_x, drift_y = drift[0:levels], drift[levels : 2 * levels]
        new_u = u + OCEAN_STEP * (rot * (v + drift_y) + turn * drift_y + mix_u)
        new_v = v + OCEAN_STEP * (-rot * (u + drift_x) - turn * drift_x + mix_v)
        target[0] = new_u
        target[1] = new_v

    half = COMM // 2
    flow(0)
    gather(0, 0)
    each(half, half + per, forward(0))
    gather(0, 1)
    each(half + per, COMM, forward(0))
    gather(0, 2)
    gather(0, 3)
    each(0, per, finish(0))
    each(0, per, lambda c: swap(1, c).start())
    each(per, COMM, finish(0))
    drift_parts(0)
    each(per, COMM, lambda c: swap(1, c).start())
    each(0, per + 1, forward(1))
    ocean(0)
    surface(state, 1)
    start(surface_pair(1))
    start(zonal_pair(1))
    each(per + 1, half, forward(1))
    flow(1)
    gather(1, 0)
    each(half, half + per, forward(1))
    gather(1, 1)
    each(half + per, COMM, forward(1))
    gather(1, 2)
    gather(1, 3)
    each(0, COMM, finish(1))
    drift_parts(1)
    ocean(1)

    sent(index_pair())
    for step in range(STEPS):
        each(0, COMM, lambda c: swap(step, c).wait_send())
        each(0, COMM, lambda c: relay(step, c).wait_send())
        sent(surface_pair(step))
        sent(zonal_pair(step))
        sent(drift_pair(step))


def local(
    spectrum, water_mask, courant, stencil_sign, quad_index, quad_weight, nonlinear, stokes_table,
    point_index, point_weight, ocean_index, ocean_weight, currents, coriolis, mixing, surface_weights,
):
    comps, points = spectrum.shape
    levels, cells = currents.shape[1:]
    f32, bf16 = jnp.float32, jnp.bfloat16
    vm = pl.BlockSpec(memory_space=pltpu.VMEM)
    dma = pltpu.SemaphoreType.DMA
    scratch = [
        pltpu.VMEM((128, comps), f32),
        pltpu.VMEM((comps, 128), f32),
        pltpu.VMEM((4, comps, comps), bf16),
        pltpu.VMEM((STEPS, comps, points), f32),
        pltpu.VMEM((STEPS, comps, points), f32),
        pltpu.VMEM((comps, points), f32),
        pltpu.VMEM((comps, points), bf16),
        pltpu.VMEM((comps, points), f32),
        pltpu.VMEM((comps, points), bf16),
        pltpu.VMEM((2, levels, cells), f32),
        pltpu.VMEM((STEPS, 8, cells), f32),
        pltpu.VMEM((STEPS, 2, 8, cells), f32),
        pltpu.VMEM((STEPS, 2, levels, cells), f32),
        pltpu.VMEM((8, cells), f32),
        pltpu.VMEM((1, 2, 8, cells), f32),
        pltpu.VMEM((3, cells, points), f32),
        pltpu.VMEM((3, points, cells), f32),
        pltpu.VMEM((STEPS, 2, 2 * levels, cells), f32),
        pltpu.VMEM((STEPS, 2, 2 * levels, cells), f32),
        pltpu.VMEM((2 * levels, cells), f32),
        pltpu.VMEM((8, points), f32),
        pltpu.VMEM((4, comps, points), f32),
        dma((STEPS, COMM)),
        dma((STEPS, COMM)),
        dma((STEPS, COMM)),
        dma((STEPS, COMM)),
    ] + [dma((n, 2)) for n in (STEPS, STEPS, STEPS, STEPS, 1, 1, STEPS, STEPS)]
    return pl.pallas_call(
        wave_kernel,
        out_shape=(
            pltpu.VMEM((comps, points), f32),
            pltpu.VMEM(currents.shape, f32),
        ),
        in_specs=[vm] * 16,
        out_specs=(vm, vm),
        scratch_shapes=scratch,
        compiler_params=pltpu.CompilerParams(
            collective_id=0, has_side_effects=True, vmem_limit_bytes=56 * 1024 * 1024
        ),
    )(
        spectrum,
        water_mask.reshape(1, points),
        courant,
        stencil_sign,
        quad_index.transpose(0, 2, 1),
        quad_weight.transpose(0, 2, 1),
        nonlinear.reshape(1, comps),
        stokes_table,
        point_index,
        point_weight,
        ocean_index,
        ocean_weight,
        currents,
        coriolis.reshape(1, cells),
        mixing.reshape(1, levels),
        surface_weights.reshape(1, levels),
    )


def solution(mesh):
    ring = P(("mp", "dev"))
    split = P(None, ("mp", "dev"))
    deep = P(None, None, ("mp", "dev"))
    return jax.shard_map(
        local,
        mesh=mesh,
        in_specs=(
            split, ring, P(), P(), P(), P(), P(), P(), split, split, split, split, deep, ring, P(), P(),
        ),
        out_specs=(split, deep),
        check_vma=False,
    )
```

```python
import jax
import jax.numpy as jnp
from jax import lax
from jax.experimental import pallas as pl
from jax.experimental.pallas import tpu as pltpu
from jax.sharding import PartitionSpec as P

STEPS = 2
OCEAN_STEP = 0.5
COMM = 8
BLOCKS = 4
MESH = pl.DeviceIdType.MESH
HIGH = lax.Precision.HIGHEST


def wave_kernel(
    spec, wet, courant, sign, qidx, qwt, nonlinear, table, pidx, pwt, oidx, owt,
    currents, coriolis, mixing, sweight,
    spec_out, cur_out,
    araw, cols, quad, near, far, adv, advb, mid, midb, state,
    sflow, shalo, zhalo, obuf, ohalo, ptab, otab, dbuf, dhalo, dself, tan,
    sem1s, sem1r, sem2s, sem2r, ssend, srecv, zsend, zrecv, osend, orecv, dsend, drecv,
):
    comps, points = spec.shape
    cells = coriolis.shape[1]
    levels = mixing.shape[1]
    dev_count = lax.axis_size("dev")
    total = lax.axis_size("mp") * dev_count
    pos = lax.axis_index("mp") * dev_count + lax.axis_index("dev")
    odd = lax.rem(pos, 2)
    up = lax.rem(pos + 1, total)
    down = lax.rem(pos + total - 1, total)
    up2 = lax.rem(pos + 2, total)
    down2 = lax.rem(pos + total - 2, total)
    partner = pos + 1 - 2 * odd
    far_to = lax.rem(pos + 2 - 4 * odd + total, total)

    def where_is(p):
        return (lax.div(p, dev_count), lax.rem(p, dev_count))

    def remote(src, dst, ssem, rsem, p):
        return pltpu.make_async_remote_copy(
            src_ref=src, dst_ref=dst, send_sem=ssem, recv_sem=rsem,
            device_id=where_is(p), device_id_type=MESH,
        )

    size = comps // COMM

    def rows(c):
        return pl.ds(pl.multiple_of(c * size, size), size)

    def swap(step, c):
        src = spec if step == 0 else mid
        return remote(src.at[rows(c)], near.at[step, rows(c)], sem1s.at[step, c], sem1r.at[step, c], partner)

    def relay(step, c):
        return remote(near.at[step, rows(c)], far.at[step, rows(c)], sem2s.at[step, c], sem2r.at[step, c], far_to)

    def pair(src_up, src_down, halo, ssem, rsem, step):
        return (
            remote(src_up, halo.at[step, 0], ssem.at[step, 0], rsem.at[step, 0], up),
            remote(src_down, halo.at[step, 1], ssem.at[step, 1], rsem.at[step, 1], down),
        )

    def surface_pair(step):
        return pair(sflow.at[step], sflow.at[step], shalo, ssend, srecv, step)

    def zonal_pair(step):
        src = currents.at[0] if step == 0 else state.at[0]
        return pair(src, src, zhalo, zsend, zrecv, step)

    def index_pair():
        return pair(obuf, obuf, ohalo, osend, orecv, 0)

    def drift_pair(step):
        return pair(dbuf.at[step, 0], dbuf.at[step, 1], dhalo, dsend, drecv, step)

    def start(copies):
        for copy in copies:
            copy.start()

    def received(copies):
        for copy in copies:
            copy.wait_recv()

    def sent(copies):
        for copy in copies:
            copy.wait_send()

    def each(low, high, body):
        def run(c, carry):
            body(c)
            return carry

        lax.fori_loop(low, high, run, 0)

    barrier = pltpu.get_barrier_semaphore()
    for p in (up, down, up2, down2):
        pl.semaphore_signal(barrier, inc=1, device_id=where_is(p), device_id_type=MESH)
    pl.semaphore_wait(barrier, 4)

    each(0, COMM, lambda c: swap(0, c).start())
    start(zonal_pair(0))
    obuf[0:4, :] = oidx[...].astype(jnp.float32)
    obuf[4:8, :] = owt[...]

    araw[...] = jnp.zeros_like(araw)
    araw[0:2, :] = courant[...]
    araw[2:4, :] = (2 * sign[...] - 1).astype(jnp.float32)
    araw[4:5, :] = nonlinear[...]
    araw[5:6, 0:levels] = mixing[...]
    araw[6:7, 0:levels] = sweight[...]
    for j in range(4):
        araw[8 + 2 * j : 10 + 2 * j, :] = qidx[j].astype(jnp.float32)
        araw[16 + 2 * j : 18 + 2 * j, :] = qwt[j]
    cols[...] = jnp.transpose(araw[...])
    sflow[...] = jnp.zeros_like(sflow)
    level_mix = cols[0:levels, 5:6]
    level_weight = cols[0:levels, 6:7]

    def surface(source, step):
        for a in range(2):
            sflow[step, a : a + 1, :] = jnp.sum(level_weight * source[a], axis=0, keepdims=True)

    surface(currents, 0)
    start(index_pair())
    start(surface_pair(0))

    lanes = lax.broadcasted_iota(jnp.int32, (32, comps), 1).astype(jnp.float32)

    def build_quad(c):
        for sub in range(size // 32):
            at = pl.ds(pl.multiple_of(c * size + sub * 32, 32), 32)
            col = cols[at, :]
            for j in range(4):
                one = jnp.where(col[:, 8 + 2 * j : 9 + 2 * j] == lanes, col[:, 16 + 2 * j : 17 + 2 * j], 0.0)
                two = jnp.where(col[:, 9 + 2 * j : 10 + 2 * j] == lanes, col[:, 17 + 2 * j : 18 + 2 * j], 0.0)
                quad[j, at, :] = (one + two).astype(jnp.bfloat16)

    def forward(step):
        def body(c):
            swap(step, c).wait_recv()
            relay(step, c).start()

        return body

    def first(c):
        build_quad(c)
        forward(0)(c)

    each(0, COMM, first)

    slots = lax.broadcasted_iota(jnp.int32, (cells, points), 0)
    for q, owner in enumerate((down, pos, up)):
        acc = jnp.zeros((cells, points), jnp.float32)
        for j in range(4):
            acc = acc + jnp.where(pidx[j : j + 1, :] - owner * cells == slots, pwt[j : j + 1, :], 0.0)
        ptab[q] = acc
    received(index_pair())
    oslots = lax.broadcasted_iota(jnp.int32, (points, cells), 0).astype(jnp.float32)
    base = (pos * points).astype(jnp.float32)
    for q in range(3):
        source = obuf[...] if q == 2 else ohalo[0, q]
        acc = jnp.zeros((points, cells), jnp.float32)
        for j in range(4):
            acc = acc + jnp.where(source[j : j + 1, :] - base == oslots, source[4 + j : 5 + j, :], 0.0)
        otab[q] = acc

    parity = (1 - 2 * odd).astype(jnp.float32)

    def flow(step):
        received(surface_pair(step))
        total_flow = jnp.dot(shalo[step, 0], ptab[0], precision=HIGH, preferred_element_type=jnp.float32)
        total_flow += jnp.dot(sflow[step], ptab[1], precision=HIGH, preferred_element_type=jnp.float32)
        total_flow += jnp.dot(shalo[step, 1], ptab[2], precision=HIGH, preferred_element_type=jnp.float32)
        tan[...] = jnp.tanh(total_flow)

    def advect(step):
        source = spec if step == 0 else mid

        def body(c):
            relay(step, c).wait_recv()
            at = rows(c)
            own = source[at, :]
            col = cols[at, :]
            sense_x = col[:, 2:3]
            sense_y = col[:, 3:4]
            behind_x = jnp.where(sense_x > 0, pltpu.roll(own, 1, 1), pltpu.roll(own, points - 1, 1))
            behind_y = jnp.where(sense_y * parity > 0, far[step, at, :], near[step, at, :])
            speed_x = col[:, 0:1] * (1.0 + 0.5 * (sense_x * tan[0:1, :]))
            speed_y = col[:, 1:2] * (1.0 + 0.5 * (sense_y * tan[1:2, :]))
            value = own - speed_x * (own - behind_x) - speed_y * (own - behind_y)
            adv[at, :] = value
            advb[at, :] = value.astype(jnp.bfloat16)

        each(0, COMM, body)

    wide = comps // BLOCKS
    wet_row = wet[...].astype(jnp.float32)

    def source_block(step):
        target = mid if step == 0 else spec_out

        def body(r):
            at = pl.ds(pl.multiple_of(r * wide, wide), wide)
            terms = [
                jnp.dot(quad[j, at, :], advb[...], preferred_element_type=jnp.float32) for j in range(4)
            ]
            value = adv[at, :]
            total_sum = terms[0] + terms[1] + terms[2] + terms[3]
            pair_sum = terms[0] * terms[1] + terms[2] * terms[3]
            new = wet_row * (value + cols[at, 4:5] * (value * value * total_sum - value * pair_sum))
            target[at, :] = new
            midb[at, :] = new.astype(jnp.bfloat16)

        return body

    def drift_parts(step):
        stokes = jnp.dot(table[...], midb[...], preferred_element_type=jnp.float32)
        ahead, behind = drift_pair(step)
        dbuf[step, 0] = jnp.dot(stokes, otab[1], precision=HIGH, preferred_element_type=jnp.float32)
        ahead.start()
        dbuf[step, 1] = jnp.dot(stokes, otab[0], precision=HIGH, preferred_element_type=jnp.float32)
        behind.start()
        dself[...] = jnp.dot(stokes, otab[2], precision=HIGH, preferred_element_type=jnp.float32)

    level_row = lax.broadcasted_iota(jnp.int32, (levels, cells), 0)

    def mix(w):
        above = jnp.where(level_row == 0, w, pltpu.roll(w, 1, 0))
        below = jnp.where(level_row == levels - 1, w, pltpu.roll(w, levels - 1, 0))
        return level_mix * (above - 2.0 * w + below)

    def ocean(step):
        source = currents if step == 0 else state
        target = state if step == 0 else cur_out
        received(zonal_pair(step))
        u, v = source[0], source[1]
        rot = coriolis[...]
        turn = 0.5 * (pltpu.roll(v, cells - 1, 1) - pltpu.roll(v, 1, 1)) - 0.5 * (zhalo[step, 1] - zhalo[step, 0])
        mix_u, mix_v = mix(u), mix(v)
        received(drift_pair(step))
        drift = dself[...] + dhalo[step, 0] + dhalo[step, 1]
        drift_x, drift_y = drift[0:levels], drift[levels : 2 * levels]
        new_u = u + OCEAN_STEP * (rot * (v + drift_y) + turn * drift_y + mix_u)
        new_v = v + OCEAN_STEP * (-rot * (u + drift_x) - turn * drift_x + mix_v)
        target[0] = new_u
        target[1] = new_v

    flow(0)
    advect(0)
    source_block(0)(0)
    per = COMM // BLOCKS
    each(0, per, lambda c: swap(1, c).start())
    each(1, BLOCKS, source_block(0))
    drift_parts(0)
    each(per, COMM, lambda c: swap(1, c).start())
    each(0, COMM - 3, forward(1))
    ocean(0)
    surface(state, 1)
    start(surface_pair(1))
    start(zonal_pair(1))
    each(COMM - 3, COMM, forward(1))
    flow(1)
    advect(1)
    each(0, BLOCKS, source_block(1))
    drift_parts(1)
    ocean(1)

    sent(index_pair())
    for step in range(STEPS):
        each(0, COMM, lambda c: swap(step, c).wait_send())
        each(0, COMM, lambda c: relay(step, c).wait_send())
        sent(surface_pair(step))
        sent(zonal_pair(step))
        sent(drift_pair(step))


def local(
    spectrum, water_mask, courant, stencil_sign, quad_index, quad_weight, nonlinear, stokes_table,
    point_index, point_weight, ocean_index, ocean_weight, currents, coriolis, mixing, surface_weights,
):
    comps, points = spectrum.shape
    levels, cells = currents.shape[1:]
    f32, bf16 = jnp.float32, jnp.bfloat16
    vm = pl.BlockSpec(memory_space=pltpu.VMEM)
    dma = pltpu.SemaphoreType.DMA
    scratch = [
        pltpu.VMEM((128, comps), f32),
        pltpu.VMEM((comps, 128), f32),
        pltpu.VMEM((4, comps, comps), bf16),
        pltpu.VMEM((STEPS, comps, points), f32),
        pltpu.VMEM((STEPS, comps, points), f32),
        pltpu.VMEM((comps, points), f32),
        pltpu.VMEM((comps, points), bf16),
        pltpu.VMEM((comps, points), f32),
        pltpu.VMEM((comps, points), bf16),
        pltpu.VMEM((2, levels, cells), f32),
        pltpu.VMEM((STEPS, 8, cells), f32),
        pltpu.VMEM((STEPS, 2, 8, cells), f32),
        pltpu.VMEM((STEPS, 2, levels, cells), f32),
        pltpu.VMEM((8, cells), f32),
        pltpu.VMEM((1, 2, 8, cells), f32),
        pltpu.VMEM((3, cells, points), f32),
        pltpu.VMEM((3, points, cells), f32),
        pltpu.VMEM((STEPS, 2, 2 * levels, cells), f32),
        pltpu.VMEM((STEPS, 2, 2 * levels, cells), f32),
        pltpu.VMEM((2 * levels, cells), f32),
        pltpu.VMEM((8, points), f32),
        dma((STEPS, COMM)),
        dma((STEPS, COMM)),
        dma((STEPS, COMM)),
        dma((STEPS, COMM)),
    ] + [dma((n, 2)) for n in (STEPS, STEPS, STEPS, STEPS, 1, 1, STEPS, STEPS)]
    return pl.pallas_call(
        wave_kernel,
        out_shape=(
            pltpu.VMEM((comps, points), f32),
            pltpu.VMEM(currents.shape, f32),
        ),
        in_specs=[vm] * 16,
        out_specs=(vm, vm),
        scratch_shapes=scratch,
        compiler_params=pltpu.CompilerParams(
            collective_id=0, has_side_effects=True, vmem_limit_bytes=56 * 1024 * 1024
        ),
    )(
        spectrum,
        water_mask.reshape(1, points),
        courant,
        stencil_sign,
        quad_index.transpose(0, 2, 1),
        quad_weight.transpose(0, 2, 1),
        nonlinear.reshape(1, comps),
        stokes_table,
        point_index,
        point_weight,
        ocean_index,
        ocean_weight,
        currents,
        coriolis.reshape(1, cells),
        mixing.reshape(1, levels),
        surface_weights.reshape(1, levels),
    )


def solution(mesh):
    ring = P(("mp", "dev"))
    split = P(None, ("mp", "dev"))
    deep = P(None, None, ("mp", "dev"))
    return jax.shard_map(
        local,
        mesh=mesh,
        in_specs=(
            split, ring, P(), P(), P(), P(), P(), P(), split, split, split, split, deep, ring, P(), P(),
        ),
        out_specs=(split, deep),
        check_vma=False,
    )
```
